64 devices in a mesh: dp: 8 (over x, y, core), tp: 8 (over z).
Axes of the slice: x: 2, y: 2, z: 8, core: 2. Of those that a mesh axis runs over, the one named last changes fastest.
The devices are a block of a 4x4x8 slice.
Arguments:
- x: bfloat16 [16384, 2048], P('dp'), parts along dimension 0
- w_gate: bfloat16 [2048, 16384], P(None, 'tp')
- w_up: bfloat16 [2048, 16384], P(None, 'tp')
- w_down: bfloat16 [16384, 2048], P('tp')
Outputs:
- output: bfloat16 [16384, 2048], P('dp'), parts along dimension 0
There are 8 independent parts. The reference program is written for one: setup_inputs(seed, part) draws one part's arguments, and reference() takes and returns one part's arrays. A program takes and returns all parts, laid end to end along the dimension named above; an argument that names none is the same for every part.
All inputs are finite; a program needn't handle non-finite values.
Results may differ from the reference program's by a relative error of at most 0.016.
Values are sent between devices in bfloat16 or wider.
A program may use at most 768 MiB of HBM per device.

```python
import jax
import jax.numpy as jnp

ROWS = 2048
D = 2048
FF = 16384


def setup_inputs(seed: int = 0, part: int = 0) -> dict:
    kx, kg, ku, kd = jax.random.split(jax.random.key(seed), 4)
    drawn = {
        "x": jax.random.normal(jax.random.fold_in(kx, part), (ROWS, D), jnp.float32),
        "w_gate": jax.random.normal(kg, (D, FF), jnp.float32) * D**-0.5,
        "w_up": jax.random.normal(ku, (D, FF), jnp.float32) * D**-0.5,
        "w_down": jax.random.normal(kd, (FF, D), jnp.float32) * FF**-0.5,
    }
    return {k: v.astype(jnp.bfloat16) for k, v in drawn.items()}


def reference(x, w_gate, w_up, w_down):
    gate = jnp.dot(x, w_gate, preferred_element_type=jnp.float32)
    up = jnp.dot(x, w_up, preferred_element_type=jnp.float32)
    hidden = (jax.nn.gelu(gate) * up).astype(jnp.bfloat16)
    return jnp.dot(hidden, w_down, preferred_element_type=jnp.float32).astype(jnp.bfloat16)
```

```python
import functools

import jax
import jax.numpy as jnp
from jax import lax
from jax.experimental import pallas as pl
from jax.experimental.pallas import tpu as pltpu
from jax.sharding import PartitionSpec as P

MESH = pl.DeviceIdType.MESH
AXIS = "tp"
PIECES = 4
HIDDEN_TILE = 256
WRITES = 8


def kernel(
    n,
    x,
    wg_hbm,
    wu_hbm,
    wd_hbm,
    y,
    wg,
    wu,
    wd,
    xs,
    hidden,
    sums,
    w_sem,
    d_sem,
    x_sem,
    send_sem,
    recv_sem,
):
    rows, depth = x.shape
    width = wg.shape[1]
    columns = wd.shape[1]
    chunk = rows // n
    half = chunk // 2
    tn = columns // PIECES
    th = HIDDEN_TILE
    tiles = width // th
    per_piece = tiles // PIECES

    me = lax.axis_index(AXIS)
    right, left = lax.rem(me + 1, n), lax.rem(me + n - 1, n)
    towards = (right, left)

    def owner(direction, step):
        if direction == 0:
            return lax.rem(me + 2 * n - step, n)
        return lax.rem(me + step, n)

    def row_of(direction, c):
        return pl.multiple_of(c * chunk + direction * half, half)

    def x_copies(step):
        slot = lax.rem(step, 2)
        return [
            pltpu.make_async_copy(
                x.at[pl.ds(row_of(d, owner(d, step)), half), :],
                xs.at[slot, pl.ds(d * half, half), :],
                x_sem.at[slot, d],
            )
            for d in range(2)
        ]

    def w_copies(j):
        cols = pl.ds(pl.multiple_of(j * th, th), th)
        return [
            pltpu.make_async_copy(wg_hbm.at[:, cols], wg.at[:, cols], w_sem.at[0, j]),
            pltpu.make_async_copy(wu_hbm.at[:, cols], wu.at[:, cols], w_sem.at[1, j]),
        ]

    def d_copy(k):
        cols = pl.ds(pl.multiple_of(k * tn, tn), tn)
        return pltpu.make_async_copy(wd_hbm.at[:, cols], wd.at[:, cols], d_sem.at[k])

    def hidden_tile(step, j):
        slot = lax.rem(step, 2)
        cols = pl.ds(pl.multiple_of(j * th, th), th)
        gate = jnp.dot(xs[slot], wg[:, cols], preferred_element_type=jnp.float32)
        up = jnp.dot(xs[slot], wu[:, cols], preferred_element_type=jnp.float32)
        hidden[slot, :, cols] = (jax.nn.gelu(gate) * up).astype(hidden.dtype)

    def term(step, k):
        slot = lax.rem(step, 2)
        cols = pl.ds(pl.multiple_of(k * tn, tn), tn)
        return jnp.dot(hidden[slot], wd[:, cols], preferred_element_type=jnp.float32)

    def reduce_copy(d, step, k):
        return pltpu.make_async_remote_copy(
            src_ref=sums.at[d, step, k],
            dst_ref=sums.at[d, step + 1, k],
            send_sem=send_sem.at[d, step, k],
            recv_sem=recv_sem.at[d, step, k],
            device_id={AXIS: towards[d]},
            device_id_type=MESH,
        )

    def gather_copy(d, hop, k):
        at = y.at[
            pl.ds(row_of(d, owner(d, n - 1 + hop)), half),
            pl.ds(pl.multiple_of(k * tn, tn), tn),
        ]
        return pltpu.make_async_remote_copy(
            src_ref=at,
            dst_ref=at,
            send_sem=send_sem.at[d, n - 1 + hop, k],
            recv_sem=recv_sem.at[d, n - 1 + hop, k],
            device_id={AXIS: towards[d]},
            device_id_type=MESH,
        )

    for copy in x_copies(0):
        copy.start()

    @pl.loop(0, tiles)
    def _(j):
        for copy in w_copies(j):
            copy.start()

    @pl.loop(0, PIECES)
    def _(k):
        d_copy(k).start()

    for copy in x_copies(1):
        copy.start()

    barrier = pltpu.get_barrier_semaphore()
    for neighbour in (left, right):
        pl.semaphore_signal(
            barrier, inc=1, device_id={AXIS: neighbour}, device_id_type=MESH
        )

    for copy in x_copies(0):
        copy.wait()

    @pl.loop(0, tiles)
    def _(j):
        for copy in w_copies(j):
            copy.wait()
        hidden_tile(0, j)

    pl.semaphore_wait(barrier, 2)

    def next_hidden(step, k):
        @pl.loop(0, per_piece)
        def _(i):
            hidden_tile(step + 1, k * per_piece + i)

    for copy in x_copies(1):
        copy.wait()

    @pl.loop(0, PIECES)
    def _(k):
        d_copy(k).wait()
        value = term(0, k).astype(sums.dtype)
        for d in range(2):
            sums[d, 0, k] = value[d * half : (d + 1) * half]
        for d in range(2):
            reduce_copy(d, 0, k).start()
        next_hidden(0, k)

    @pl.loop(1, n - 1)
    def _(step):
        for copy in x_copies(step + 1):
            copy.start()
        for copy in x_copies(step + 1):
            copy.wait()

        @pl.loop(0, PIECES)
        def _(k):
            value = term(step, k)
            for d in range(2):
                reduce_copy(d, step - 1, k).wait_recv()
                part = value[d * half : (d + 1) * half]
                sums[d, step, k] = (
                    sums[d, step, k].astype(jnp.float32) + part
                ).astype(sums.dtype)
                reduce_copy(d, step, k).start()
            next_hidden(step, k)

    @pl.loop(0, PIECES)
    def _(k):
        value = term(n - 1, k)
        for d in range(2):
            reduce_copy(d, n - 2, k).wait_recv()
            part = value[d * half : (d + 1) * half]
            y[
                pl.ds(row_of(d, owner(d, n - 1)), half),
                pl.ds(pl.multiple_of(k * tn, tn), tn),
            ] = (sums[d, n - 1, k].astype(jnp.float32) + part).astype(y.dtype)
            gather_copy(d, 0, k).start()

    @pl.loop(1, n - 1)
    def _(hop):
        @pl.loop(0, PIECES)
        def _(k):
            for d in range(2):
                gather_copy(d, hop - 1, k).wait_recv()
                gather_copy(d, hop, k).start()

    @pl.loop(0, PIECES)
    def _(k):
        for d in range(2):
            gather_copy(d, n - 2, k).wait_recv()

    @pl.loop(0, n - 1)
    def _(step):
        @pl.loop(0, PIECES)
        def _(k):
            for d in range(2):
                reduce_copy(d, step, k).wait_send()
                gather_copy(d, step, k).wait_send()


def write_out(y, out, sem):
    rows = y.shape[0] // WRITES
    copies = [
        pltpu.make_async_copy(
            y.at[pl.ds(i * rows, rows), :], out.at[pl.ds(i * rows, rows), :], sem.at[i]
        )
        for i in range(WRITES)
    ]
    for copy in copies:
        copy.start()
    for copy in copies:
        copy.wait()


def solution(mesh):
    n = mesh.shape[AXIS]

    def step(x, w_gate, w_up, w_down):
        rows, depth = x.shape
        width, columns = w_down.shape
        chunk = rows // n
        half = chunk // 2
        tn = columns // PIECES
        tiles = width // HIDDEN_TILE
        dtype = x.dtype
        hbm = pl.BlockSpec(memory_space=pltpu.HBM)
        gathered = pl.pallas_call(
            functools.partial(kernel, n),
            out_shape=jax.ShapeDtypeStruct((rows, columns), dtype),
            in_specs=[hbm] * 4,
            out_specs=pl.BlockSpec(memory_space=pltpu.VMEM),
            scratch_shapes=[
                pltpu.VMEM(w_gate.shape, dtype),
                pltpu.VMEM(w_up.shape, dtype),
                pltpu.VMEM(w_down.shape, dtype),
                pltpu.VMEM((2, chunk, depth), dtype),
                pltpu.VMEM((2, chunk, width), dtype),
                pltpu.VMEM((2, n, PIECES, half, tn), dtype),
                pltpu.SemaphoreType.DMA((2, tiles)),
                pltpu.SemaphoreType.DMA((PIECES,)),
                pltpu.SemaphoreType.DMA((2, 2)),
                pltpu.SemaphoreType.DMA((2, 2 * n - 2, PIECES)),
                pltpu.SemaphoreType.DMA((2, 2 * n - 2, PIECES)),
            ],
            compiler_params=pltpu.CompilerParams(
                collective_id=0,
                has_side_effects=True,
                vmem_limit_bytes=45 * 1024 * 1024,
            ),
            cost_estimate=pl.CostEstimate(
                flops=6 * rows * depth * width,
                bytes_accessed=2 * (rows * depth * 2 + 3 * depth * width),
                transcendentals=rows * width,
            ),
            name="mlp_ring",
        )(x, w_gate, w_up, w_down)
        return pl.pallas_call(
            write_out,
            out_shape=jax.ShapeDtypeStruct((rows, columns), dtype),
            in_specs=[pl.BlockSpec(memory_space=pltpu.VMEM)],
            out_specs=hbm,
            scratch_shapes=[pltpu.SemaphoreType.DMA((WRITES,))],
            compiler_params=pltpu.CompilerParams(vmem_limit_bytes=12 * 1024 * 1024),
            name="write_out",
        )(gathered)

    return jax.shard_map(
        step,
        mesh=mesh,
        in_specs=(P("dp", None), P(None, AXIS), P(None, AXIS), P(AXIS, None)),
        out_specs=P("dp", None),
        check_vma=False,
    )
```

```python
import functools

import jax
import jax.numpy as jnp
from jax import lax
from jax.experimental import pallas as pl
from jax.experimental.pallas import tpu as pltpu
from jax.sharding import PartitionSpec as P

MESH = pl.DeviceIdType.MESH
AXIS = "tp"
PIECES = 4
HIDDEN_TILE = 512
FIRST_TILES = 4
WRITES = 8


def kernel(
    n,
    x,
    wg_hbm,
    wu_hbm,
    wd_hbm,
    y,
    wg,
    wu,
    wd,
    xs,
    hidden,
    sums,
    w_sem,
    d_sem,
    x_sem,
    recv_sem,
    credit_sem,
):
    rows, depth = x.shape
    width = wg.shape[1]
    columns = wd.shape[1]
    chunk = rows // n
    half = chunk // 2
    tn = columns // PIECES
    th = HIDDEN_TILE
    tiles = width // th
    per_piece = tiles // PIECES
    tw = width // FIRST_TILES
    last = 2 * n - 3
    send_sem = w_sem

    me = lax.axis_index(AXIS)
    right, left = lax.rem(me + 1, n), lax.rem(me + n - 1, n)
    towards = (right, left)

    def owner(direction, step):
        if direction == 0:
            return lax.rem(me + 2 * n - step, n)
        return lax.rem(me + step, n)

    def row_of(direction, c):
        return pl.multiple_of(c * chunk + direction * half, half)

    def x_copies(step):
        slot = lax.rem(step, 2)
        return [
            pltpu.make_async_copy(
                x.at[pl.ds(row_of(d, owner(d, step)), half), :],
                xs.at[slot, pl.ds(d * half, half), :],
                x_sem.at[slot, d],
            )
            for d in range(2)
        ]

    def w_copies(j):
        cols = pl.ds(pl.multiple_of(j * tw, tw), tw)
        return [
            pltpu.make_async_copy(wg_hbm.at[:, cols], wg.at[:, cols], w_sem.at[0, j]),
            pltpu.make_async_copy(wu_hbm.at[:, cols], wu.at[:, cols], w_sem.at[1, j]),
        ]

    def d_copy(k):
        cols = pl.ds(pl.multiple_of(k * tn, tn), tn)
        return pltpu.make_async_copy(wd_hbm.at[:, cols], wd.at[:, cols], d_sem.at[k])

    def hidden_tile(step, j):
        slot = lax.rem(step, 2)
        cols = pl.ds(pl.multiple_of(j * th, th), th)
        gate = jnp.dot(xs[slot], wg[:, cols], preferred_element_type=jnp.float32)
        up = jnp.dot(xs[slot], wu[:, cols], preferred_element_type=jnp.float32)
        hidden[slot, :, cols] = (jax.nn.gelu(gate) * up).astype(hidden.dtype)

    def term(step, k):
        slot = lax.rem(step, 2)
        cols = pl.ds(pl.multiple_of(k * tn, tn), tn)
        return jnp.dot(hidden[slot], wd[:, cols], preferred_element_type=jnp.float32)

    def message(d, m, k, src, dst):
        return pltpu.make_async_remote_copy(
            src_ref=src,
            dst_ref=dst,
            send_sem=send_sem.at[d, k],
            recv_sem=recv_sem.at[d, lax.rem(m, 2), k],
            device_id={AXIS: towards[d]},
            device_id_type=MESH,
        )

    def reduce_copy(d, step, k):
        return message(d, step, k, sums.at[d, step, k], sums.at[d, step + 1, k])

    def gather_copy(d, hop, k):
        at = y.at[
            pl.ds(row_of(d, owner(d, n - 1 + hop)), half),
            pl.ds(pl.multiple_of(k * tn, tn), tn),
        ]
        return message(d, n - 1 + hop, k, at, at)

    def give_credit(d, k):
        pl.semaphore_signal(
            credit_sem.at[d, k],
            inc=1,
            device_id={AXIS: towards[1 - d]},
            device_id_type=MESH,
        )

    def take_credit(d, k):
        pl.semaphore_wait(credit_sem.at[d, k], 1)

    for copy in x_copies(0):
        copy.start()

    @pl.loop(0, FIRST_TILES)
    def _(j):
        for copy in w_copies(j):
            copy.start()

    @pl.loop(0, PIECES)
    def _(k):
        d_copy(k).start()

        @pl.when(k == 0)
        def _():
            for copy in x_copies(1):
                copy.start()

    barrier = pltpu.get_barrier_semaphore()
    for neighbour in (left, right):
        pl.semaphore_signal(
            barrier, inc=1, device_id={AXIS: neighbour}, device_id_type=MESH
        )

    for copy in x_copies(0):
        copy.wait()

    @pl.loop(0, FIRST_TILES)
    def _(j):
        for copy in w_copies(j):
            copy.wait()
        hidden_tile(0, j)

    pl.semaphore_wait(barrier, 2)

    def next_hidden(step, k):
        @pl.loop(0, per_piece)
        def _(i):
            hidden_tile(step + 1, k * per_piece + i)

    @pl.loop(0, PIECES)
    def _(k):
        d_copy(k).wait()
        value = term(0, k).astype(sums.dtype)
        for d in range(2):
            sums[d, 0, k] = value[d * half : (d + 1) * half]
        for d in range(2):
            reduce_copy(d, 0, k).start()

        @pl.when(k == 0)
        def _():
            for copy in x_copies(1):
                copy.wait()

        next_hidden(0, k)

    for copy in x_copies(2):
        copy.start()

    @pl.loop(1, n - 1)
    def _(step):
        for copy in x_copies(step + 1):
            copy.wait()

        @pl.loop(0, PIECES)
        def _(k):
            value = term(step, k)
            for d in range(2):
                reduce_copy(d, step - 1, k).wait()
                give_credit(d, k)
                part = value[d * half : (d + 1) * half]
                sums[d, step, k] = (
                    sums[d, step, k].astype(jnp.float32) + part
                ).astype(sums.dtype)

                @pl.when(step >= 2)
                def _():
                    take_credit(d, k)

                reduce_copy(d, step, k).start()
            next_hidden(step, k)

        @pl.when(step < n - 2)
        def _():
            for copy in x_copies(step + 2):
                copy.start()

    @pl.loop(0, PIECES)
    def _(k):
        value = term(n - 1, k)
        for d in range(2):
            reduce_copy(d, n - 2, k).wait()
            give_credit(d, k)
            part = value[d * half : (d + 1) * half]
            y[
                pl.ds(row_of(d, owner(d, n - 1)), half),
                pl.ds(pl.multiple_of(k * tn, tn), tn),
            ] = (sums[d, n - 1, k].astype(jnp.float32) + part).astype(y.dtype)
            take_credit(d, k)
            gather_copy(d, 0, k).start()

    @pl.loop(1, n - 1)
    def _(hop):
        @pl.loop(0, PIECES)
        def _(k):
            for d in range(2):
                gather_copy(d, hop - 1, k).wait()
                take_credit(d, k)
                gather_copy(d, hop, k).start()

                @pl.when(n - 1 + hop - 1 <= last - 2)
                def _():
                    give_credit(d, k)

    @pl.loop(0, PIECES)
    def _(k):
        for d in range(2):
            gather_copy(d, n - 2, k).wait()


def write_out(y, out, sem):
    rows = y.shape[0] // WRITES
    copies = [
        pltpu.make_async_copy(
            y.at[pl.ds(i * rows, rows), :], out.at[pl.ds(i * rows, rows), :], sem.at[i]
        )
        for i in range(WRITES)
    ]
    for copy in copies:
        copy.start()
    for copy in copies:
        copy.wait()


def solution(mesh):
    n = mesh.shape[AXIS]

    def step(x, w_gate, w_up, w_down):
        rows, depth = x.shape
        width, columns = w_down.shape
        chunk = rows // n
        half = chunk // 2
        tn = columns // PIECES
        dtype = x.dtype
        hbm = pl.BlockSpec(memory_space=pltpu.HBM)
        gathered = pl.pallas_call(
            functools.partial(kernel, n),
            out_shape=jax.ShapeDtypeStruct((rows, columns), dtype),
            in_specs=[hbm] * 4,
            out_specs=pl.BlockSpec(memory_space=pltpu.VMEM),
            scratch_shapes=[
                pltpu.VMEM(w_gate.shape, dtype),
                pltpu.VMEM(w_up.shape, dtype),
                pltpu.VMEM(w_down.shape, dtype),
                pltpu.VMEM((2, chunk, depth), dtype),
                pltpu.VMEM((2, chunk, width), dtype),
                pltpu.VMEM((2, n, PIECES, half, tn), dtype),
                pltpu.SemaphoreType.DMA((2, FIRST_TILES)),
                pltpu.SemaphoreType.DMA((PIECES,)),
                pltpu.SemaphoreType.DMA((2, 2)),
                pltpu.SemaphoreType.DMA((2, 2, PIECES)),
                pltpu.SemaphoreType.REGULAR((2, PIECES)),
            ],
            compiler_params=pltpu.CompilerParams(
                collective_id=0,
                has_side_effects=True,
                vmem_limit_bytes=45 * 1024 * 1024,
            ),
            cost_estimate=pl.CostEstimate(
                flops=6 * rows * depth * width,
                bytes_accessed=2 * (rows * depth * 2 + 3 * depth * width),
                transcendentals=rows * width,
            ),
            name="mlp_ring",
        )(x, w_gate, w_up, w_down)
        return pl.pallas_call(
            write_out,
            out_shape=jax.ShapeDtypeStruct((rows, columns), dtype),
            in_specs=[pl.BlockSpec(memory_space=pltpu.VMEM)],
            out_specs=hbm,
            scratch_shapes=[pltpu.SemaphoreType.DMA((WRITES,))],
            compiler_params=pltpu.CompilerParams(vmem_limit_bytes=12 * 1024 * 1024),
            name="write_out",
        )(gathered)

    return jax.shard_map(
        step,
        mesh=mesh,
        in_specs=(P("dp", None), P(None, AXIS), P(None, AXIS), P(AXIS, None)),
        out_specs=P("dp", None),
        check_vma=False,
    )
```

```python
import functools

import jax
import jax.numpy as jnp
from jax import lax
from jax.experimental import pallas as pl
from jax.experimental.pallas import tpu as pltpu
from jax.sharding import PartitionSpec as P

MESH = pl.DeviceIdType.MESH
AXIS = "tp"
PARTS = 2
PIECES = 2
SHARES = 2
FIRST_TILES = 4
WRITES = 4


def kernel(
    n,
    x,
    wg_hbm,
    wu_hbm,
    wd_hbm,
    y,
    wg,
    wu,
    wd,
    xs,
    hidden,
    sums,
    w_sem,
    d_sem,
    x_sem,
    recv_sem,
    credit_sem,
):
    rows, depth = x.shape
    width = wg.shape[1]
    columns = wd.shape[1]
    chunk = rows // n
    half = chunk // 2
    part = half // PARTS
    units = n * PARTS
    tn = columns // PIECES
    tw = width // FIRST_TILES
    th = width // PIECES
    tf = tn // SHARES
    firsts = PIECES * SHARES
    last = 2 * n - 3
    send_sem = w_sem

    me = lax.axis_index(AXIS)
    right, left = lax.rem(me + 1, n), lax.rem(me + n - 1, n)
    towards = (right, left)

    def owner(direction, step):
        if direction == 0:
            return lax.rem(me + 2 * n - step, n)
        return lax.rem(me + step, n)

    def row_of(direction, step, p):
        row = owner(direction, step) * chunk + direction * half + p * part
        return pl.multiple_of(row, part)

    def columns_of(k, size=tn):
        return pl.ds(pl.multiple_of(k * size, size), size)

    def x_copies(unit):
        slot = lax.rem(unit, 2)
        step, p = lax.div(unit, PARTS), lax.rem(unit, PARTS)
        return [
            pltpu.make_async_copy(
                x.at[pl.ds(row_of(d, step, p), part), :],
                xs.at[slot, pl.ds(d * part, part), :],
                x_sem.at[slot, d],
            )
            for d in range(2)
        ]

    def w_copies(j):
        cols = pl.ds(pl.multiple_of(j * tw, tw), tw)
        return [
            pltpu.make_async_copy(wg_hbm.at[:, cols], wg.at[:, cols], w_sem.at[0, j]),
            pltpu.make_async_copy(wu_hbm.at[:, cols], wu.at[:, cols], w_sem.at[1, j]),
        ]

    def d_copy(k):
        cols = columns_of(k, tf)
        return pltpu.make_async_copy(wd_hbm.at[:, cols], wd.at[:, cols], d_sem.at[k])

    def hidden_tile(unit, j, size):
        slot = lax.rem(unit, 2)
        cols = pl.ds(pl.multiple_of(j * size, size), size)
        gate = jnp.dot(xs[slot], wg[:, cols], preferred_element_type=jnp.float32)
        up = jnp.dot(xs[slot], wu[:, cols], preferred_element_type=jnp.float32)
        hidden[slot, :, cols] = (jax.nn.gelu(gate) * up).astype(hidden.dtype)

    def term(unit, cols):
        slot = lax.rem(unit, 2)
        return jnp.dot(hidden[slot], wd[:, cols], preferred_element_type=jnp.float32)

    def message(d, m, p, k, src, dst):
        piece = p * PIECES + k
        return pltpu.make_async_remote_copy(
            src_ref=src,
            dst_ref=dst,
            send_sem=send_sem.at[d, piece],
            recv_sem=recv_sem.at[d, lax.rem(m, 2), piece],
            device_id={AXIS: towards[d]},
            device_id_type=MESH,
        )

    def reduce_copy(d, step, p, k):
        return message(
            d, step, p, k, sums.at[d, step, p, k], sums.at[d, step + 1, p, k]
        )

    def first_copy(d, p, k, share):
        cols = columns_of(share, tf)
        return message(
            d, 0, p, k, sums.at[d, 0, p, k, :, cols], sums.at[d, 1, p, k, :, cols]
        )

    def gather_copy(d, hop, p, k):
        at = y.at[pl.ds(row_of(d, n - 1 + hop, p), part), columns_of(k)]
        return message(d, n - 1 + hop, p, k, at, at)

    def give_credit(d):
        pl.semaphore_signal(
            credit_sem.at[d],
            inc=1,
            device_id={AXIS: towards[1 - d]},
            device_id_type=MESH,
        )

    def take_credit(d):
        pl.semaphore_wait(credit_sem.at[d], 1)

    for copy in x_copies(0):
        copy.start()

    @pl.loop(0, FIRST_TILES)
    def _(j):
        for copy in w_copies(j):
            copy.start()

    @pl.loop(0, firsts)
    def _(k):
        d_copy(k).start()

        @pl.when(k == 0)
        def _():
            for copy in x_copies(1):
                copy.start()

    barrier = pltpu.get_barrier_semaphore()
    for neighbour in (left, right):
        pl.semaphore_signal(
            barrier, inc=1, device_id={AXIS: neighbour}, device_id_type=MESH
        )

    for copy in x_copies(0):
        copy.wait()

    @pl.loop(0, FIRST_TILES)
    def _(j):
        for copy in w_copies(j):
            copy.wait()
        hidden_tile(0, j, tw)

    pl.semaphore_wait(barrier, 2)

    def next_hidden(unit, k, size=th):
        @pl.when(k == 0)
        def _():
            for copy in x_copies(unit + 1):
                copy.wait()

        hidden_tile(unit + 1, k, size)

    def fetch(unit):
        for copy in x_copies(unit):
            copy.start()

    @pl.loop(0, PARTS)
    def _(unit):
        @pl.loop(0, firsts)
        def _(f):
            k, share = lax.div(f, SHARES), lax.rem(f, SHARES)

            @pl.when(unit == 0)
            def _():
                d_copy(f).wait()

            value = term(unit, columns_of(f, tf)).astype(sums.dtype)
            for d in range(2):
                sums[d, 0, unit, k, :, columns_of(share, tf)] = value[
                    d * part : (d + 1) * part
                ]
            for d in range(2):
                first_copy(d, unit, k, share).start()
            next_hidden(unit, f, width // firsts)

            @pl.when(f == 0)
            def _():
                fetch(unit + 2)

    @pl.loop(PARTS, units - PARTS)
    def _(unit):
        step, p = lax.div(unit, PARTS), lax.rem(unit, PARTS)

        fetch(unit + 2)

        @pl.loop(0, PIECES)
        def _(k):
            value = term(unit, columns_of(k))
            for d in range(2):
                reduce_copy(d, step - 1, p, k).wait()
                give_credit(d)
                sums[d, step, p, k] = (
                    sums[d, step, p, k].astype(jnp.float32)
                    + value[d * part : (d + 1) * part]
                ).astype(sums.dtype)

                @pl.when(step >= 2)
                def _():
                    take_credit(d)

                reduce_copy(d, step, p, k).start()
            next_hidden(unit, k)

    @pl.loop(units - PARTS, units)
    def _(unit):
        p = lax.rem(unit, PARTS)

        @pl.loop(0, PIECES)
        def _(k):
            value = term(unit, columns_of(k))
            for d in range(2):
                reduce_copy(d, n - 2, p, k).wait()
                give_credit(d)
                y[pl.ds(row_of(d, n - 1, p), part), columns_of(k)] = (
                    sums[d, n - 1, p, k].astype(jnp.float32)
                    + value[d * part : (d + 1) * part]
                ).astype(y.dtype)
                take_credit(d)
                gather_copy(d, 0, p, k).start()

            @pl.when(unit < units - 1)
            def _():
                next_hidden(unit, k)

    @pl.loop(1, n - 1)
    def _(hop):
        @pl.loop(0, PARTS)
        def _(p):
            @pl.loop(0, PIECES)
            def _(k):
                for d in range(2):
                    gather_copy(d, hop - 1, p, k).wait()
                    take_credit(d)
                    gather_copy(d, hop, p, k).start()

                    @pl.when(n - 1 + hop - 1 <= last - 2)
                    def _():
                        give_credit(d)

    @pl.loop(0, PARTS)
    def _(p):
        @pl.loop(0, PIECES)
        def _(k):
            for d in range(2):
                gather_copy(d, n - 2, p, k).wait()


def write_out(y, out, sem):
    rows = y.shape[0] // WRITES
    copies = [
        pltpu.make_async_copy(
            y.at[pl.ds(i * rows, rows), :], out.at[pl.ds(i * rows, rows), :], sem.at[i]
        )
        for i in range(WRITES)
    ]
    for copy in copies:
        copy.start()
    for copy in copies:
        copy.wait()


def solution(mesh):
    n = mesh.shape[AXIS]

    def step(x, w_gate, w_up, w_down):
        rows, depth = x.shape
        width, columns = w_down.shape
        half = rows // n // 2
        part = half // PARTS
        tn = columns // PIECES
        dtype = x.dtype
        hbm = pl.BlockSpec(memory_space=pltpu.HBM)
        gathered = pl.pallas_call(
            functools.partial(kernel, n),
            out_shape=jax.ShapeDtypeStruct((rows, columns), dtype),
            in_specs=[hbm] * 4,
            out_specs=pl.BlockSpec(memory_space=pltpu.VMEM),
            scratch_shapes=[
                pltpu.VMEM(w_gate.shape, dtype),
                pltpu.VMEM(w_up.shape, dtype),
                pltpu.VMEM(w_down.shape, dtype),
                pltpu.VMEM((2, 2 * part, depth), dtype),
                pltpu.VMEM((2, 2 * part, width), dtype),
                pltpu.VMEM((2, n, PARTS, PIECES, part, tn), dtype),
                pltpu.SemaphoreType.DMA((2, FIRST_TILES)),
                pltpu.SemaphoreType.DMA((PIECES * SHARES,)),
                pltpu.SemaphoreType.DMA((2, 2)),
                pltpu.SemaphoreType.DMA((2, 2, PARTS * PIECES)),
                pltpu.SemaphoreType.REGULAR((2,)),
            ],
            compiler_params=pltpu.CompilerParams(
                collective_id=0,
                has_side_effects=True,
                vmem_limit_bytes=45 * 1024 * 1024,
            ),
            cost_estimate=pl.CostEstimate(
                flops=6 * rows * depth * width,
                bytes_accessed=2 * (rows * depth * 2 + 3 * depth * width),
                transcendentals=rows * width,
            ),
            name="mlp_ring",
        )(x, w_gate, w_up, w_down)
        return pl.pallas_call(
            write_out,
            out_shape=jax.ShapeDtypeStruct((rows, columns), dtype),
            in_specs=[pl.BlockSpec(memory_space=pltpu.VMEM)],
            out_specs=hbm,
            scratch_shapes=[pltpu.SemaphoreType.DMA((WRITES,))],
            compiler_params=pltpu.CompilerParams(vmem_limit_bytes=12 * 1024 * 1024),
            name="write_out",
        )(gathered)

    return jax.shard_map(
        step,
        mesh=mesh,
        in_specs=(P("dp", None), P(None, AXIS), P(None, AXIS), P(AXIS, None)),
        out_specs=P("dp", None),
        check_vma=False,
    )
```

```python
import functools

import jax
import jax.numpy as jnp
from jax import lax
from jax.experimental import pallas as pl
from jax.experimental.pallas import tpu as pltpu
from jax.sharding import PartitionSpec as P

MESH = pl.DeviceIdType.MESH
AXIS = "tp"
PARTS = 2
PIECES = 1
SHARES = 4
FIRST_TILES = 8
WRITES = 4


def kernel(
    n,
    x,
    wg_hbm,
    wu_hbm,
    wd_hbm,
    y,
    wg,
    wu,
    wd,
    xs,
    hidden,
    sums,
    w_sem,
    d_sem,
    x_sem,
    recv_sem,
    credit_sem,
):
    rows, depth = x.shape
    width = wg.shape[1]
    columns = wd.shape[1]
    chunk = rows // n
    half = chunk // 2
    part = half // PARTS
    units = n * PARTS
    tn = columns // PIECES
    tw = width // FIRST_TILES
    th = width // 2
    tf = tn // SHARES
    firsts = PIECES * SHARES
    last = 2 * n - 3
    send_sem = w_sem

    me = lax.axis_index(AXIS)
    right, left = lax.rem(me + 1, n), lax.rem(me + n - 1, n)
    towards = (right, left)

    def owner(direction, step):
        if direction == 0:
            return lax.rem(me + 2 * n - step, n)
        return lax.rem(me + step, n)

    def row_of(direction, step, p):
        row = owner(direction, step) * chunk + direction * half + p * part
        return pl.multiple_of(row, part)

    def columns_of(k, size=tn):
        return pl.ds(pl.multiple_of(k * size, size), size)

    def x_copies(unit):
        slot = lax.rem(unit, 2)
        step, p = lax.div(unit, PARTS), lax.rem(unit, PARTS)
        return [
            pltpu.make_async_copy(
                x.at[pl.ds(row_of(d, step, p), part), :],
                xs.at[slot, pl.ds(d * part, part), :],
                x_sem.at[slot, d],
            )
            for d in range(2)
        ]

    def w_copies(j):
        cols = pl.ds(pl.multiple_of(j * tw, tw), tw)
        return [
            pltpu.make_async_copy(wg_hbm.at[:, cols], wg.at[:, cols], w_sem.at[0, j]),
            pltpu.make_async_copy(wu_hbm.at[:, cols], wu.at[:, cols], w_sem.at[1, j]),
        ]

    def d_copy(k, size=tf):
        cols = columns_of(k, size)
        sem = d_sem.at[k] if size == tf else d_sem.at[k * firsts]
        return pltpu.make_async_copy(wd_hbm.at[:, cols], wd.at[:, cols], sem)

    def hidden_tile(unit, j, size):
        slot = lax.rem(unit, 2)
        cols = pl.ds(pl.multiple_of(j * size, size), size)
        gate = jnp.dot(xs[slot], wg[:, cols], preferred_element_type=jnp.float32)
        up = jnp.dot(xs[slot], wu[:, cols], preferred_element_type=jnp.float32)
        hidden[slot, :, cols] = (jax.nn.gelu(gate) * up).astype(hidden.dtype)

    def term(unit, cols):
        slot = lax.rem(unit, 2)
        return jnp.dot(hidden[slot], wd[:, cols], preferred_element_type=jnp.float32)

    def message(d, m, p, k, src, dst):
        piece = p * PIECES + k
        return pltpu.make_async_remote_copy(
            src_ref=src,
            dst_ref=dst,
            send_sem=send_sem.at[d, piece],
            recv_sem=recv_sem.at[d, lax.rem(m, 2), piece],
            device_id={AXIS: towards[d]},
            device_id_type=MESH,
        )

    def reduce_copy(d, step, p, k):
        return message(
            d, step, p, k, sums.at[d, step, p, k], sums.at[d, step + 1, p, k]
        )

    def first_copy(d, p, k, share, size=tf):
        cols = columns_of(share, size)
        return message(
            d, 0, p, k, sums.at[d, 0, p, k, :, cols], sums.at[d, 1, p, k, :, cols]
        )

    def gather_copy(d, hop, p, k):
        at = y.at[pl.ds(row_of(d, n - 1 + hop, p), part), columns_of(k)]
        return message(d, n - 1 + hop, p, k, at, at)

    def give_credit(d):
        pl.semaphore_signal(
            credit_sem.at[d],
            inc=1,
            device_id={AXIS: towards[1 - d]},
            device_id_type=MESH,
        )

    def take_credit(d):
        pl.semaphore_wait(credit_sem.at[d], 1)

    for copy in x_copies(0):
        copy.start()

    @pl.loop(0, FIRST_TILES)
    def _(j):
        for copy in w_copies(j):
            copy.start()

    @pl.loop(0, 2)
    def _(k):
        d_copy(k, tf // 2).start()

    for copy in x_copies(1):
        copy.start()

    @pl.loop(1, firsts)
    def _(k):
        d_copy(k).start()

    barrier = pltpu.get_barrier_semaphore()
    for neighbour in (left, right):
        pl.semaphore_signal(
            barrier, inc=1, device_id={AXIS: neighbour}, device_id_type=MESH
        )

    for copy in x_copies(0):
        copy.wait()

    @pl.loop(0, FIRST_TILES)
    def _(j):
        for copy in w_copies(j):
            copy.wait()
        hidden_tile(0, j, tw)

    pl.semaphore_wait(barrier, 2)

    def next_hidden(unit, k, size=th):
        @pl.when(k == 0)
        def _():
            for copy in x_copies(unit + 1):
                copy.wait()

        hidden_tile(unit + 1, k, size)

    def fetch(unit):
        for copy in x_copies(unit):
            copy.start()

    @pl.loop(0, 2)
    def _(f):
        d_copy(f, tf // 2).wait()
        value = term(0, columns_of(f, tf // 2)).astype(sums.dtype)
        for d in range(2):
            sums[d, 0, 0, 0, :, columns_of(f, tf // 2)] = value[
                d * part : (d + 1) * part
            ]
        for d in range(2):
            first_copy(d, 0, 0, f, tf // 2).start()

    fetch(2)

    @pl.loop(0, PARTS)
    def _(unit):
        @pl.loop(jnp.where(unit == 0, 1, 0), firsts)
        def _(f):
            k, share = lax.div(f, SHARES), lax.rem(f, SHARES)

            @pl.when(unit == 0)
            def _():
                d_copy(f).wait()

            value = term(unit, columns_of(f, tf)).astype(sums.dtype)
            for d in range(2):
                sums[d, 0, unit, k, :, columns_of(share, tf)] = value[
                    d * part : (d + 1) * part
                ]
            for d in range(2):
                first_copy(d, unit, k, share).start()
            next_hidden(unit, jnp.where(unit == 0, f - 1, f), width // firsts)

            @pl.when(f == 0)
            def _():
                fetch(unit + 2)

        @pl.when(unit == 0)
        def _():
            next_hidden(unit, jnp.int32(firsts - 1), width // firsts)

    @pl.loop(PARTS, units - PARTS)
    def _(unit):
        step, p = lax.div(unit, PARTS), lax.rem(unit, PARTS)

        fetch(unit + 2)

        @pl.loop(0, PIECES)
        def _(k):
            value = term(unit, columns_of(k))
            for d in range(2):
                reduce_copy(d, step - 1, p, k).wait()
                give_credit(d)
                sums[d, step, p, k] = (
                    sums[d, step, p, k].astype(jnp.float32)
                    + value[d * part : (d + 1) * part]
                ).astype(sums.dtype)

                @pl.when(step >= 2)
                def _():
                    take_credit(d)

                reduce_copy(d, step, p, k).start()
            for tile in range(2):
                next_hidden(unit, jnp.int32(tile))

    @pl.loop(units - PARTS, units)
    def _(unit):
        p = lax.rem(unit, PARTS)

        @pl.loop(0, PIECES)
        def _(k):
            value = term(unit, columns_of(k))
            for d in range(2):
                reduce_copy(d, n - 2, p, k).wait()
                give_credit(d)
                y[pl.ds(row_of(d, n - 1, p), part), columns_of(k)] = (
                    sums[d, n - 1, p, k].astype(jnp.float32)
                    + value[d * part : (d + 1) * part]
                ).astype(y.dtype)
                take_credit(d)
                gather_copy(d, 0, p, k).start()

            @pl.when(unit < units - 1)
            def _():
                for tile in range(2):
                    next_hidden(unit, jnp.int32(tile))

    @pl.loop(1, n - 1)
    def _(hop):
        @pl.loop(0, PARTS)
        def _(p):
            @pl.loop(0, PIECES)
            def _(k):
                for d in range(2):
                    gather_copy(d, hop - 1, p, k).wait()
                    take_credit(d)
                    gather_copy(d, hop, p, k).start()

                    @pl.when(n - 1 + hop - 1 <= last - 2)
                    def _():
                        give_credit(d)

    @pl.loop(0, PARTS)
    def _(p):
        @pl.loop(0, PIECES)
        def _(k):
            for d in range(2):
                gather_copy(d, n - 2, p, k).wait()


def write_out(y, out, sem):
    rows = y.shape[0] // WRITES
    copies = [
        pltpu.make_async_copy(
            y.at[pl.ds(i * rows, rows), :], out.at[pl.ds(i * rows, rows), :], sem.at[i]
        )
        for i in range(WRITES)
    ]
    for copy in copies:
        copy.start()
    for copy in copies:
        copy.wait()


def solution(mesh):
    n = mesh.shape[AXIS]

    def step(x, w_gate, w_up, w_down):
        rows, depth = x.shape
        width, columns = w_down.shape
        half = rows // n // 2
        part = half // PARTS
        tn = columns // PIECES
        dtype = x.dtype
        hbm = pl.BlockSpec(memory_space=pltpu.HBM)
        gathered = pl.pallas_call(
            functools.partial(kernel, n),
            out_shape=jax.ShapeDtypeStruct((rows, columns), dtype),
            in_specs=[hbm] * 4,
            out_specs=pl.BlockSpec(memory_space=pltpu.VMEM),
            scratch_shapes=[
                pltpu.VMEM(w_gate.shape, dtype),
                pltpu.VMEM(w_up.shape, dtype),
                pltpu.VMEM(w_down.shape, dtype),
                pltpu.VMEM((2, 2 * part, depth), dtype),
                pltpu.VMEM((2, 2 * part, width), dtype),
                pltpu.VMEM((2, n, PARTS, PIECES, part, tn), dtype),
                pltpu.SemaphoreType.DMA((2, FIRST_TILES)),
                pltpu.SemaphoreType.DMA((PIECES * SHARES + 1,)),
                pltpu.SemaphoreType.DMA((2, 2)),
                pltpu.SemaphoreType.DMA((2, 2, PARTS * PIECES)),
                pltpu.SemaphoreType.REGULAR((2,)),
            ],
            compiler_params=pltpu.CompilerParams(
                collective_id=0,
                has_side_effects=True,
                vmem_limit_bytes=45 * 1024 * 1024,
            ),
            cost_estimate=pl.CostEstimate(
                flops=6 * rows * depth * width,
                bytes_accessed=2 * (rows * depth * 2 + 3 * depth * width),
                transcendentals=rows * width,
            ),
            name="mlp_ring",
        )(x, w_gate, w_up, w_down)
        return pl.pallas_call(
            write_out,
            out_shape=jax.ShapeDtypeStruct((rows, columns), dtype),
            in_specs=[pl.BlockSpec(memory_space=pltpu.VMEM)],
            out_specs=hbm,
            scratch_shapes=[pltpu.SemaphoreType.DMA((WRITES,))],
            compiler_params=pltpu.CompilerParams(vmem_limit_bytes=12 * 1024 * 1024),
            name="write_out",
        )(gathered)

    return jax.shard_map(
        step,
        mesh=mesh,
        in_specs=(P("dp", None), P(None, AXIS), P(None, AXIS), P(AXIS, None)),
        out_specs=P("dp", None),
        check_vma=False,
    )
```

```python
import functools

import jax
import jax.numpy as jnp
from jax import lax
from jax.experimental import pallas as pl
from jax.experimental.pallas import tpu as pltpu
from jax.sharding import PartitionSpec as P

MESH = pl.DeviceIdType.MESH
AXIS = "tp"
PARTS = 2
PIECES = 1
SHARES = 4
FIRST_TILES = 8
WRITES = 4


def kernel(
    n,
    x,
    wg_hbm,
    wu_hbm,
    wd_hbm,
    y,
    wgu,
    wd,
    xs,
    hidden,
    sums,
    w_sem,
    d_sem,
    x_sem,
    recv_sem,
    credit_sem,
):
    rows, depth = x.shape
    width = wd.shape[0]
    columns = wd.shape[1]
    chunk = rows // n
    half = chunk // 2
    part = half // PARTS
    units = n * PARTS
    tn = columns // PIECES
    tw = width // FIRST_TILES
    th = width // 2
    tf = tn // SHARES
    firsts = PIECES * SHARES
    last = 2 * n - 3
    wg, wu = wgu.at[0], wgu.at[1]
    send_sem = w_sem

    me = lax.axis_index(AXIS)
    right, left = lax.rem(me + 1, n), lax.rem(me + n - 1, n)
    towards = (right, left)

    def owner(direction, step):
        if direction == 0:
            return lax.rem(me + 2 * n - step, n)
        return lax.rem(me + step, n)

    def row_of(direction, step, p):
        row = owner(direction, step) * chunk + direction * half + p * part
        return pl.multiple_of(row, part)

    def columns_of(k, size=tn):
        return pl.ds(pl.multiple_of(k * size, size), size)

    def x_copies(unit):
        slot = lax.rem(unit, 2)
        step, p = lax.div(unit, PARTS), lax.rem(unit, PARTS)
        return [
            pltpu.make_async_copy(
                x.at[pl.ds(row_of(d, step, p), part), :],
                xs.at[slot, pl.ds(d * part, part), :],
                x_sem.at[slot, d],
            )
            for d in range(2)
        ]

    def w_copies(j):
        cols = pl.ds(pl.multiple_of(j * tw, tw), tw)
        return [
            pltpu.make_async_copy(wg_hbm.at[:, cols], wg.at[:, cols], w_sem.at[j]),
            pltpu.make_async_copy(wu_hbm.at[:, cols], wu.at[:, cols], w_sem.at[j]),
        ]

    def w_wait(j):
        both = wgu.at[:, :, pl.ds(pl.multiple_of(j * tw, tw), tw)]
        pltpu.make_async_copy(both, both, w_sem.at[j]).wait()

    def d_copy(k, size=tf):
        cols = columns_of(k, size)
        sem = d_sem.at[k] if size == tf else d_sem.at[k * firsts]
        return pltpu.make_async_copy(wd_hbm.at[:, cols], wd.at[:, cols], sem)

    def hidden_tile(unit, j, size):
        slot = lax.rem(unit, 2)
        cols = pl.ds(pl.multiple_of(j * size, size), size)
        gate = jnp.dot(xs[slot], wg[:, cols], preferred_element_type=jnp.float32)
        up = jnp.dot(xs[slot], wu[:, cols], preferred_element_type=jnp.float32)
        hidden[slot, :, cols] = (jax.nn.gelu(gate) * up).astype(hidden.dtype)

    def term(unit, cols):
        slot = lax.rem(unit, 2)
        return jnp.dot(hidden[slot], wd[:, cols], preferred_element_type=jnp.float32)

    def message(d, m, p, k, src, dst):
        piece = p * PIECES + k
        return pltpu.make_async_remote_copy(
            src_ref=src,
            dst_ref=dst,
            send_sem=send_sem.at[d * PARTS * PIECES + piece],
            recv_sem=recv_sem.at[d, lax.rem(m, 2), piece],
            device_id={AXIS: towards[d]},
            device_id_type=MESH,
        )

    def reduce_copy(d, step, p, k):
        return message(
            d, step, p, k, sums.at[d, step, p, k], sums.at[d, step + 1, p, k]
        )

    def first_copy(d, p, k, share, size=tf):
        cols = columns_of(share, size)
        return message(
            d, 0, p, k, sums.at[d, 0, p, k, :, cols], sums.at[d, 1, p, k, :, cols]
        )

    def gather_copy(d, hop, p, k):
        at = y.at[pl.ds(row_of(d, n - 1 + hop, p), part), columns_of(k)]
        return message(d, n - 1 + hop, p, k, at, at)

    def give_credit(d):
        pl.semaphore_signal(
            credit_sem.at[d],
            inc=1,
            device_id={AXIS: towards[1 - d]},
            device_id_type=MESH,
        )

    def take_credit(d):
        pl.semaphore_wait(credit_sem.at[d], 1)

    for copy in x_copies(0):
        copy.start()

    @pl.loop(0, FIRST_TILES)
    def _(j):
        for copy in w_copies(j):
            copy.start()

    @pl.loop(0, 2)
    def _(k):
        d_copy(k, tf // 2).start()

    for copy in x_copies(1):
        copy.start()

    @pl.loop(1, firsts)
    def _(k):
        d_copy(k).start()

    barrier = pltpu.get_barrier_semaphore()
    for neighbour in (left, right):
        pl.semaphore_signal(
            barrier, inc=1, device_id={AXIS: neighbour}, device_id_type=MESH
        )

    for copy in x_copies(0):
        copy.wait()

    @pl.loop(0, FIRST_TILES)
    def _(j):
        w_wait(j)
        hidden_tile(0, j, tw)

    pl.semaphore_wait(barrier, 2)

    def next_hidden(unit, k, size=th):
        @pl.when(k == 0)
        def _():
            for copy in x_copies(unit + 1):
                copy.wait()

        hidden_tile(unit + 1, k, size)

    def fetch(unit):
        for copy in x_copies(unit):
            copy.start()

    @pl.loop(0, 2)
    def _(f):
        d_copy(f, tf // 2).wait()
        value = term(0, columns_of(f, tf // 2)).astype(sums.dtype)
        for d in range(2):
            sums[d, 0, 0, 0, :, columns_of(f, tf // 2)] = value[
                d * part : (d + 1) * part
            ]
        for d in range(2):
            first_copy(d, 0, 0, f, tf // 2).start()

    fetch(2)

    @pl.loop(0, PARTS)
    def _(unit):
        @pl.loop(jnp.where(unit == 0, 1, 0), firsts)
        def _(f):
            k, share = lax.div(f, SHARES), lax.rem(f, SHARES)

            @pl.when(unit == 0)
            def _():
                d_copy(f).wait()

            value = term(unit, columns_of(f, tf)).astype(sums.dtype)
            for d in range(2):
                sums[d, 0, unit, k, :, columns_of(share, tf)] = value[
                    d * part : (d + 1) * part
                ]
            for d in range(2):
                first_copy(d, unit, k, share).start()
            next_hidden(unit, jnp.where(unit == 0, f - 1, f), width // firsts)

            @pl.when(f == 0)
            def _():
                fetch(unit + 2)

        @pl.when(unit == 0)
        def _():
            next_hidden(unit, jnp.int32(firsts - 1), width // firsts)

    @pl.loop(PARTS, units - PARTS)
    def _(unit):
        step, p = lax.div(unit, PARTS), lax.rem(unit, PARTS)

        fetch(unit + 2)

        @pl.loop(0, PIECES)
        def _(k):
            value = term(unit, columns_of(k))
            for d in range(2):
                reduce_copy(d, step - 1, p, k).wait()
                give_credit(d)
                sums[d, step, p, k] = (
                    sums[d, step, p, k].astype(jnp.float32)
                    + value[d * part : (d + 1) * part]
                ).astype(sums.dtype)

                @pl.when(step >= 2)
                def _():
                    take_credit(d)

                reduce_copy(d, step, p, k).start()
            for tile in range(2):
                next_hidden(unit, jnp.int32(tile))

    @pl.loop(units - PARTS, units)
    def _(unit):
        p = lax.rem(unit, PARTS)

        @pl.loop(0, PIECES)
        def _(k):
            value = term(unit, columns_of(k))
            for d in range(2):
                reduce_copy(d, n - 2, p, k).wait()
                give_credit(d)
                y[pl.ds(row_of(d, n - 1, p), part), columns_of(k)] = (
                    sums[d, n - 1, p, k].astype(jnp.float32)
                    + value[d * part : (d + 1) * part]
                ).astype(y.dtype)
                take_credit(d)
                gather_copy(d, 0, p, k).start()

            @pl.when(unit < units - 1)
            def _():
                for tile in range(2):
                    next_hidden(unit, jnp.int32(tile))

    @pl.loop(1, n - 1)
    def _(hop):
        @pl.loop(0, PARTS)
        def _(p):
            @pl.loop(0, PIECES)
            def _(k):
                for d in range(2):
                    gather_copy(d, hop - 1, p, k).wait()
                    take_credit(d)
                    gather_copy(d, hop, p, k).start()

                    @pl.when(n - 1 + hop - 1 <= last - 2)
                    def _():
                        give_credit(d)

    @pl.loop(0, PARTS)
    def _(p):
        @pl.loop(0, PIECES)
        def _(k):
            for d in range(2):
                gather_copy(d, n - 2, p, k).wait()


def write_out(y, out, sem):
    rows = y.shape[0] // WRITES
    copies = [
        pltpu.make_async_copy(
            y.at[pl.ds(i * rows, rows), :], out.at[pl.ds(i * rows, rows), :], sem.at[i]
        )
        for i in range(WRITES)
    ]
    for copy in copies:
        copy.start()
    for copy in copies:
        copy.wait()


def solution(mesh):
    n = mesh.shape[AXIS]

    def step(x, w_gate, w_up, w_down):
        rows, depth = x.shape
        width, columns = w_down.shape
        half = rows // n // 2
        part = half // PARTS
        tn = columns // PIECES
        dtype = x.dtype
        hbm = pl.BlockSpec(memory_space=pltpu.HBM)
        gathered = pl.pallas_call(
            functools.partial(kernel, n),
            out_shape=jax.ShapeDtypeStruct((rows, columns), dtype),
            in_specs=[hbm] * 4,
            out_specs=pl.BlockSpec(memory_space=pltpu.VMEM),
            scratch_shapes=[
                pltpu.VMEM((2, *w_gate.shape), dtype),
                pltpu.VMEM(w_down.shape, dtype),
                pltpu.VMEM((2, 2 * part, depth), dtype),
                pltpu.VMEM((2, 2 * part, width), dtype),
                pltpu.VMEM((2, n, PARTS, PIECES, part, tn), dtype),
                pltpu.SemaphoreType.DMA((FIRST_TILES,)),
                pltpu.SemaphoreType.DMA((PIECES * SHARES + 1,)),
                pltpu.SemaphoreType.DMA((2, 2)),
                pltpu.SemaphoreType.DMA((2, 2, PARTS * PIECES)),
                pltpu.SemaphoreType.REGULAR((2,)),
            ],
            compiler_params=pltpu.CompilerParams(
                collective_id=0,
                has_side_effects=True,
                vmem_limit_bytes=45 * 1024 * 1024,
            ),
            cost_estimate=pl.CostEstimate(
                flops=6 * rows * depth * width,
                bytes_accessed=2 * (rows * depth * 2 + 3 * depth * width),
                transcendentals=rows * width,
            ),
            name="mlp_ring",
        )(x, w_gate, w_up, w_down)
        return pl.pallas_call(
            write_out,
            out_shape=jax.ShapeDtypeStruct((rows, columns), dtype),
            in_specs=[pl.BlockSpec(memory_space=pltpu.VMEM)],
            out_specs=hbm,
            scratch_shapes=[pltpu.SemaphoreType.DMA((WRITES,))],
            compiler_params=pltpu.CompilerParams(vmem_limit_bytes=12 * 1024 * 1024),
            name="write_out",
        )(gathered)

    return jax.shard_map(
        step,
        mesh=mesh,
        in_specs=(P("dp", None), P(None, AXIS), P(None, AXIS), P(AXIS, None)),
        out_specs=P("dp", None),
        check_vma=False,
    )
```
